32 devices in a mesh: section: 4 (over z), shard: 8 (over y, x, core).
Axes of the slice: x: 2, y: 2, z: 4, core: 2. Of those that a mesh axis runs over, the one named last changes fastest.
Arguments:
- grad_parts: bfloat16 [4, 8, 256, 8192], P('section', 'shard'), may hold values from -6 to 6
- params: bfloat16 [4, 256, 8192], P('section', 'shard'), may hold values from -6 to 6
- moment_first: float32 [4, 256, 8192], P('section', 'shard'), may hold values from -6 to 6
- moment_second: float32 [4, 256, 8192], P('section', 'shard'), may hold values from 0.5 to 50
- block_layer: int32 [4, 32], P('section', 'shard'), may hold values from 0 to 7, as said below
- block_valid: int32 [4, 32], P('section', 'shard'), may hold values from 0 to 1
- decay: float32 [8], replicated, may hold values from 0.05 to 1
Outputs:
- new_params: bfloat16 [4, 256, 8192], P('section', 'shard')
- new_first: float32 [4, 256, 8192], P('section', 'shard')
- new_second: float32 [4, 256, 8192], P('section', 'shard')
- ratios: float32 [8], replicated
The draws below stay inside these ranges and needn't reach their ends.
Inputs may be any that keep to these rules, and one draw needn't show every extreme that they name: `block_layer`: in every section the live slots come first. One section has all 32 slots live; each other section has between 16 and 32 live slots, and all sections together have 3 * 32. Over the live slots taken section by section in order, layer ids never fall and every layer has exactly 12 live slots; dead slots hold arbitrary layer ids.
All inputs are finite; a program needn't handle non-finite values.
Results may differ from the reference program's by a relative error of at most 0.008.
Values may be sent and summed in bfloat16 or wider, within the bound.
No kernel may reach another device: no remote copies, remote signals or barrier semaphores. Data moves between devices by JAX's collectives and lax.ppermute only.
A program may use at most 64 MiB of HBM per device.

```python
import math
import jax
import jax.numpy as jnp
from jax import lax

D = 8192
LAYERS = 8
BLOCK = 8
SECTION_BLK = 32
SECTION_ROWS = 256
LAYER_BLK = 12
N_SECTION = 4
N_SHARD = 8


def layout(key):
    keyed = jax.random.fold_in(key, 11)
    full = SECTION_BLK
    half_blk = SECTION_BLK // 2
    first_count = jax.random.randint(jax.random.fold_in(keyed, 3), (), half_blk, full + 1)
    lower = jnp.maximum(half_blk, full - first_count)
    upper = jnp.minimum(full, 3 * half_blk - first_count)
    second_count = jax.random.randint(jax.random.fold_in(keyed, 4), (), lower, upper + 1)
    third_count = 2 * full - first_count - second_count
    base = jnp.stack([jnp.array(full, jnp.int32), first_count.astype(jnp.int32), second_count.astype(jnp.int32), third_count.astype(jnp.int32)])
    order = jax.random.permutation(jax.random.fold_in(keyed, 1), 4)
    counts = base[order]
    offsets = jnp.cumsum(counts) - counts
    slots = jnp.arange(SECTION_BLK, dtype=jnp.int32)
    valid = slots[None, :] < counts[:, None]
    position = offsets[:, None] + slots[None, :]
    layer = position // LAYER_BLK
    filler = jax.random.randint(jax.random.fold_in(keyed, 2), (4, SECTION_BLK), 0, LAYERS)
    return (jnp.where(valid, layer, filler).astype(jnp.int32), valid.astype(jnp.int32))


def draw_block_layer(key, part):
    return layout(key)[0]


def draw_block_valid(key, part):
    return layout(key)[1]


def strengthened(result, key, source, target, blocks, factor):
    owner, partner = [(jnp.arange(result.shape[dim]) // (result.shape[dim] // blocks)).reshape([-1 if axis == dim else 1 for axis in range(result.ndim)]) for dim in (source, target)]
    chosen = jax.random.permutation(key, blocks)[partner]
    strong = (owner == chosen) | (owner == (partner + blocks // 2) % blocks)
    return jnp.where(strong, factor * result, result)


def level_of(own_key, shape, shards, least, top_value):
    factor_of, own = 1.0, jax.random.fold_in(own_key, 6)
    for axis_at, blocks in shards:
        heights = jnp.exp(jax.random.uniform(jax.random.fold_in(own, axis_at), (blocks,), jnp.float32, least / len(shards), top_value / len(shards)))
        factor_of = factor_of * jnp.repeat(heights, shape[axis_at] // blocks).reshape([-1 if axis == axis_at else 1 for axis in range(len(shape))])
    return factor_of


def centred(stream_key, shape, spread, bound, split=(), kind=jnp.bfloat16):
    loudness = level_of(stream_key, shape, split, -0.22, 0.18) if split else 1.0
    result = jax.random.normal(stream_key, shape, jnp.float32) * spread * loudness
    return jnp.minimum(jnp.maximum(result, -bound), bound).astype(kind)


def noise_with(key, dims, width, bound, pieces, heavy, kind=jnp.bfloat16):
    entries = width * jax.random.normal(key, dims, jnp.float32)
    if pieces:
        entries = entries * level_of(key, dims, pieces, -0.22, 0.18)
    return jnp.clip(strengthened(entries, jax.random.fold_in(key, 3), *heavy), -bound, bound).astype(kind)


def setup_inputs(seed: int = 0) -> dict:
    seeds = jax.random.split(jax.random.key(seed), 8)
    return {
        "grad_parts": noise_with(seeds[0], (N_SECTION, N_SHARD, SECTION_ROWS, D), 1.0, 6.0, ((0, 4), (1, 8)), (1, 2, 8, 2.0)),
        "params": centred(seeds[1], (N_SECTION, SECTION_ROWS, D), 1.0, 6.0, ((0, 4), (1, 8))),
        "moment_first": centred(seeds[2], (N_SECTION, SECTION_ROWS, D), 1.0, 6.0, ((0, 4), (1, 8)), jnp.float32),
        "moment_second": jnp.clip(jnp.exp(math.log(50.0) - 4.6051702 * jax.random.uniform(seeds[3], (N_SECTION, SECTION_ROWS, D), jnp.float32) ** level_of(seeds[3], (N_SECTION, SECTION_ROWS, D), ((0, 4), (1, 8)), -0.2, 0.2)), 0.5, 50.0),
        "block_layer": draw_block_layer(jax.random.fold_in(seeds[7], 71), 0),
        "block_valid": draw_block_valid(jax.random.fold_in(seeds[7], 71), 0),
        "decay": jnp.clip(jnp.exp(jax.random.uniform(seeds[6], (LAYERS,), jnp.float32, math.log(0.05), math.log(1.0))), 0.05, 1.0),
    }


bias_first = 1.0 - 0.9 ** 10
bias_second = 1.0 - 0.99 ** 10

def reference(grad_parts, params, moment_first, moment_second, block_layer, block_valid, decay):

    def add_part(index, running):
        return running + lax.dynamic_index_in_dim(grad_parts, index, 1, keepdims=False).astype(jnp.float32)
    initial = jnp.zeros((grad_parts.shape[0], grad_parts.shape[2], grad_parts.shape[3]), jnp.float32)
    gradient = lax.fori_loop(0, grad_parts.shape[1], add_part, initial)
    first = 0.9 * moment_first + 0.1 * gradient
    second = 0.99 * moment_second + 0.01 * gradient * gradient
    layer_rows = jnp.repeat(block_layer, BLOCK, axis=1)
    valid_rows = jnp.repeat(block_valid, BLOCK, axis=1) > 0
    weights = params.astype(jnp.float32)
    update = first / bias_first / (jnp.sqrt(second / bias_second) + 1e-06) + decay[layer_rows][..., None] * weights
    onehot = jnp.where(valid_rows[..., None] & (layer_rows[..., None] == jnp.arange(LAYERS, dtype=jnp.int32)), 1.0, 0.0).astype(jnp.float32)
    weight_sq = lax.optimization_barrier(jnp.sum(weights * weights, axis=-1))
    update_sq = lax.optimization_barrier(jnp.sum(update * update, axis=-1))
    wsum = jnp.einsum('sr,srl->l', weight_sq, onehot, precision=lax.Precision.HIGHEST)
    usum = jnp.einsum('sr,srl->l', update_sq, onehot, precision=lax.Precision.HIGHEST)
    ratios = jnp.sqrt(wsum / (usum + 1.0))
    row_ratio = ratios[layer_rows]
    stepped = weights - 0.1 * row_ratio[..., None] * update
    new_params = jnp.where(valid_rows[..., None], stepped, weights).astype(jnp.bfloat16)
    new_first = jnp.where(valid_rows[..., None], first, moment_first)
    new_second = jnp.where(valid_rows[..., None], second, moment_second)
    return (new_params, new_first, new_second, ratios)
```

```python
import jax
import jax.numpy as jnp
from jax import lax
from jax.sharding import PartitionSpec as P

bias_first = 1.0 - 0.9**10
bias_second = 1.0 - 0.99**10


def bits_of(size):
    return size.bit_length() - 1


def reversed_bits(value, bits):
    return sum(((value >> b) & 1) << (bits - 1 - b) for b in range(bits))


def swapped(size, distance_of):
    return [(i, i ^ distance_of(i)) for i in range(size)]


def scattered_sum(parts, count, rows):
    me = lax.axis_index("shard")
    core = me & 1
    chip = me >> 1
    bits = bits_of(count // 2)
    chips = 1 << bits

    def block(r, to_core):
        away = jnp.where(to_core == 0, r, reversed_bits(r, bits))
        owner = ((chip ^ away) << 1) | to_core
        return lax.dynamic_slice_in_dim(parts, owner * rows, rows, 0)

    total = [None] * chips
    for r in reversed(range(chips)):
        from_partner = lax.ppermute(block(r, 1 - core), "shard", swapped(count, lambda i: 1))
        total[r] = block(r, core).astype(jnp.float32) + from_partner.astype(jnp.float32)
    for b in reversed(range(bits)):
        step = 1 << b
        pairs = swapped(
            count, lambda i: (step if i & 1 == 0 else 1 << (bits - 1 - b)) << 1
        )
        for r in reversed(range(step, 2 * step)):
            sent = total[r].astype(jnp.bfloat16)
            received = lax.ppermute(sent, "shard", pairs)
            total[r - step] = total[r - step] + received.astype(jnp.float32)
    return total[0]


def summed_everywhere(value, axis, size):
    for b in range(bits_of(size)):
        value = value + lax.ppermute(value, axis, swapped(size, lambda i: 1 << b))
    return value


def shards(grad_parts, params, moment_first, moment_second, block_layer, block_valid, decay):
    row_count = params.shape[1]
    n_shard = lax.axis_size("shard")
    n_section = lax.axis_size("section")
    gradient = scattered_sum(grad_parts[0, 0], n_shard, row_count)
    block_rows = row_count // block_layer.shape[1]
    layer_rows = jnp.repeat(block_layer[0], block_rows)
    valid_rows = jnp.repeat(block_valid[0], block_rows) > 0
    layer_ids = jnp.arange(decay.shape[0], dtype=jnp.int32)
    onehot = jnp.where(
        valid_rows[:, None] & (layer_rows[:, None] == layer_ids[None, :]), 1.0, 0.0
    ).astype(jnp.float32)
    weights = params[0].astype(jnp.float32)
    first = 0.9 * moment_first[0] + 0.1 * gradient
    second = 0.99 * moment_second[0] + 0.01 * gradient * gradient
    row_decay = jnp.dot(onehot, decay, precision=lax.Precision.HIGHEST)
    update = (
        first / bias_first / (jnp.sqrt(second / bias_second) + 1e-06) + row_decay[:, None] * weights
    )
    row_sums = jnp.stack(
        [jnp.sum(weights * weights, axis=-1), jnp.sum(update * update, axis=-1)], axis=1
    )
    partial_value = jnp.dot(onehot.T, row_sums, precision=lax.Precision.HIGHEST)
    totals = summed_everywhere(partial_value, "shard", n_shard)
    totals = summed_everywhere(totals, "section", n_section)
    ratios = jnp.sqrt(totals[:, 0] / (totals[:, 1] + 1.0))
    row_ratio = jnp.dot(onehot, ratios, precision=lax.Precision.HIGHEST)
    stepped = weights - 0.1 * row_ratio[:, None] * update
    live = valid_rows[:, None]
    new_params = jnp.where(live, stepped, weights).astype(jnp.bfloat16)
    new_first = jnp.where(live, first, moment_first[0])
    new_second = jnp.where(live, second, moment_second[0])
    return (new_params[None], new_first[None], new_second[None], ratios)


def solution(mesh):
    placed = (
        P("section", "shard", None, None),
        P("section", "shard", None),
        P("section", "shard", None),
        P("section", "shard", None),
        P("section", "shard"),
        P("section", "shard"),
        P(),
    )
    return jax.shard_map(
        shards,
        mesh=mesh,
        in_specs=placed,
        out_specs=(
            P("section", "shard", None),
            P("section", "shard", None),
            P("section", "shard", None),
            P(),
        ),
        check_vma=False,
    )
```

```python
import jax
import jax.numpy as jnp
from jax import lax
from jax.experimental import pallas as pl
from jax.experimental.pallas import tpu as pltpu
from jax.sharding import PartitionSpec as P

bias_first = 1.0 - 0.9**10
bias_second = 1.0 - 0.99**10

vmem_bytes = 3 << 19


def bits_of(size):
    return size.bit_length() - 1


def reversed_bits(value, bits):
    return sum(((value >> b) & 1) << (bits - 1 - b) for b in range(bits))


def swapped(size, distance_of):
    return [(i, i ^ distance_of(i)) for i in range(size)]


def after(value, *earlier):
    return lax.optimization_barrier((value, *earlier))[0]


def owner_of(me, r, to_core, bits):
    away = jnp.where(to_core == 0, r, reversed_bits(r, bits))
    return (((me >> 1) ^ away) << 1) | to_core


def partner_rows(parts, me, chosen, rows, bits):
    def copies(me_ref, parts_ref, *refs):
        outs, sems = refs[: len(chosen)], refs[len(chosen)]
        own_index = me_ref[0]
        started = []
        for g, r in enumerate(chosen):
            owner = owner_of(own_index, r, 1 - (own_index & 1), bits)
            source = parts_ref.at[pl.ds(pl.multiple_of(owner * rows, rows), rows)]
            started.append(pltpu.make_async_copy(source, outs[g], sems.at[g]))
        for copy in started:
            copy.start()
        for copy in started:
            copy.wait()

    shape = (rows, parts.shape[1])
    moved = 4 * len(chosen) * shape[0] * shape[1]
    return pl.pallas_call(
        copies,
        out_shape=[pltpu.VMEM(shape, parts.dtype)] * len(chosen),
        in_specs=[
            pl.BlockSpec(memory_space=pltpu.SMEM),
            pl.BlockSpec(memory_space=pl.ANY),
        ],
        out_specs=[pl.BlockSpec(memory_space=pltpu.VMEM)] * len(chosen),
        scratch_shapes=[pltpu.SemaphoreType.DMA((len(chosen),))],
        cost_estimate=pl.CostEstimate(flops=0, transcendentals=0, bytes_accessed=moved),
    )(me.reshape(1), parts)


def scattered_sum(parts, count, rows):
    me = lax.axis_index("shard")
    core = me & 1
    bits = bits_of(count // 2)
    chips = 1 << bits

    def block(r, to_core, held):
        return lax.dynamic_slice_in_dim(held, owner_of(me, r, to_core, bits) * rows, rows, 0)

    def exchanged(away):
        return lax.ppermute(away, "shard", swapped(count, lambda i: 1))

    def core_sum(r):
        return block(r, core, parts).astype(jnp.float32) + partner[r].astype(jnp.float32)

    last = chips - 1
    (away_last,) = partner_rows(parts, me, (last,), rows, bits)
    partner = {last: exchanged(away_last)}
    later = after(parts, away_last)
    in_vmem = min(last, vmem_bytes // (rows * parts.shape[1] * parts.dtype.itemsize))
    chosen = tuple(range(last - 1, last - 1 - in_vmem, -1))
    away = dict(zip(chosen, partner_rows(later, me, chosen, rows, bits)))
    for r in reversed(range(last)):
        partner[r] = exchanged(away[r] if r in away else block(r, 1 - core, later))

    received = {}
    for r in reversed(range(chips)):
        total = core_sum(r)
        arrivals = received.pop(r, [])
        if r == 0:
            for arrival in arrivals[:-1]:
                total = total + arrival.astype(jnp.float32)
            return after(total) + arrivals[-1].astype(jnp.float32)
        for arrival in arrivals:
            total = total + arrival.astype(jnp.float32)
        b = r.bit_length() - 1
        pairs = swapped(
            count, lambda i: (1 << b if i & 1 == 0 else 1 << (bits - 1 - b)) << 1
        )
        sent = total.astype(jnp.bfloat16)
        partner[r - 1] = after(partner[r - 1], sent)
        arrival = lax.ppermute(sent, "shard", pairs)
        received.setdefault(r - (1 << b), []).append(arrival)


def summed_over(value, axis, distance):
    size = lax.axis_size(axis)
    return value + lax.ppermute(value, axis, swapped(size, lambda i: distance))


def step(grad_parts, params, moment_first, moment_second, block_layer, block_valid, decay):
    row_count = params.shape[1]
    n_shard = lax.axis_size("shard")
    n_section = lax.axis_size("section")
    gradient = scattered_sum(grad_parts[0, 0], n_shard, row_count)
    block_rows = row_count // block_layer.shape[1]
    layer_rows = jnp.repeat(block_layer[0], block_rows)
    valid_rows = jnp.repeat(block_valid[0], block_rows) > 0
    layer_ids = jnp.arange(decay.shape[0], dtype=jnp.int32)
    onehot = jnp.where(
        valid_rows[:, None] & (layer_rows[:, None] == layer_ids[None, :]), 1.0, 0.0
    ).astype(jnp.float32)
    weights = params[0].astype(jnp.float32)
    weight_sums = after(jnp.sum(weights * weights, axis=-1))
    row_decay = after(jnp.dot(onehot, decay, precision=lax.Precision.HIGHEST))
    first = 0.9 * moment_first[0] + 0.1 * gradient
    second = 0.99 * moment_second[0] + 0.01 * gradient * gradient
    update = (
        first / bias_first / (jnp.sqrt(second / bias_second) + 1e-06) + row_decay[:, None] * weights
    )
    row_sums = jnp.stack([weight_sums, jnp.sum(update * update, axis=-1)], axis=1)
    partial_value = jnp.dot(onehot.T, row_sums, precision=lax.Precision.HIGHEST)
    late_gradient = after(gradient, partial_value)
    live = valid_rows[:, None]
    first = 0.9 * moment_first[0] + 0.1 * late_gradient
    second = 0.99 * moment_second[0] + 0.01 * late_gradient * late_gradient
    new_first = jnp.where(live, first, moment_first[0])
    new_second = jnp.where(live, second, moment_second[0])
    totals = partial_value
    hops = [("shard", 1 << b) for b in range(bits_of(n_shard))]
    hops += [("section", 1 << b) for b in range(bits_of(n_section))]
    for at, (axis, distance) in enumerate(hops):
        totals = summed_over(totals, axis, distance)
        if at == 1:
            totals, new_first, new_second = lax.optimization_barrier(
                (totals, new_first, new_second)
            )
    ratios = jnp.sqrt(totals[:, 0] / (totals[:, 1] + 1.0))
    row_ratio = jnp.dot(onehot, ratios, precision=lax.Precision.HIGHEST)
    stepped = weights - 0.1 * row_ratio[:, None] * update
    new_params = jnp.where(live, stepped, weights).astype(jnp.bfloat16)
    return (new_params[None], new_first[None], new_second[None], ratios)


def solution(mesh):
    placed = (
        P("section", "shard", None, None),
        P("section", "shard", None),
        P("section", "shard", None),
        P("section", "shard", None),
        P("section", "shard"),
        P("section", "shard"),
        P(),
    )
    return jax.shard_map(
        step,
        mesh=mesh,
        in_specs=placed,
        out_specs=(
            P("section", "shard", None),
            P("section", "shard", None),
            P("section", "shard", None),
            P(),
        ),
        check_vma=False,
    )
```

```python
import jax
import jax.numpy as jnp
from jax import lax
from jax.experimental import pallas as pl
from jax.experimental.pallas import tpu as pltpu
from jax.sharding import PartitionSpec as P


bias_first = 1.0 - 0.9**10
bias_second = 1.0 - 0.99**10

vmem_bytes = 3 << 19


def bits_of(size):
    return size.bit_length() - 1


def reversed_bits(value, bits):
    return sum(((value >> b) & 1) << (bits - 1 - b) for b in range(bits))


def swapped(size, distance_of):
    return [(i, i ^ distance_of(i)) for i in range(size)]


def after(value, *earlier):
    return lax.optimization_barrier((value, *earlier))[0]


def owner_of(me, r, to_core, bits):
    away = jnp.where(to_core == 0, r, reversed_bits(r, bits))
    return (((me >> 1) ^ away) << 1) | to_core


def partner_rows(parts, me, chosen, rows, bits):
    def copies(me_ref, parts_ref, *refs):
        outs, sems = refs[: len(chosen)], refs[len(chosen)]
        own_index = me_ref[0]
        started = []
        for g, r in enumerate(chosen):
            owner = owner_of(own_index, r, 1 - (own_index & 1), bits)
            source = parts_ref.at[pl.ds(pl.multiple_of(owner * rows, rows), rows)]
            started.append(pltpu.make_async_copy(source, outs[g], sems.at[g]))
        for copy in started:
            copy.start()
        for copy in started:
            copy.wait()

    shape = (rows, parts.shape[1])
    moved = 4 * len(chosen) * shape[0] * shape[1]
    return pl.pallas_call(
        copies,
        out_shape=[pltpu.VMEM(shape, parts.dtype)] * len(chosen),
        in_specs=[
            pl.BlockSpec(memory_space=pltpu.SMEM),
            pl.BlockSpec(memory_space=pl.ANY),
        ],
        out_specs=[pl.BlockSpec(memory_space=pltpu.VMEM)] * len(chosen),
        scratch_shapes=[pltpu.SemaphoreType.DMA((len(chosen),))],
        cost_estimate=pl.CostEstimate(flops=0, transcendentals=0, bytes_accessed=moved),
    )(me.reshape(1), parts)


def scattered_sum(parts, count, rows):
    me = lax.axis_index("shard")
    core = me & 1
    bits = bits_of(count // 2)
    chips = 1 << bits

    def block(r, to_core, held):
        return lax.dynamic_slice_in_dim(held, owner_of(me, r, to_core, bits) * rows, rows, 0)

    def exchanged(away):
        return lax.ppermute(away, "shard", swapped(count, lambda i: 1))

    def core_sum(r):
        return block(r, core, parts).astype(jnp.float32) + partner[r].astype(jnp.float32)

    last = chips - 1
    (away_last,) = partner_rows(parts, me, (last,), rows, bits)
    partner = {last: exchanged(away_last)}
    later = after(parts, away_last)
    in_vmem = min(last, vmem_bytes // (rows * parts.shape[1] * parts.dtype.itemsize))
    chosen = tuple(range(last - 1, last - 1 - in_vmem, -1))
    away = dict(zip(chosen, partner_rows(later, me, chosen, rows, bits)))
    lead = core_sum(last).astype(jnp.bfloat16)
    for r in reversed(range(last)):
        waiting = away[r] if r in away else block(r, 1 - core, later)
        partner[r] = exchanged(after(waiting, lead))

    received = {}
    for r in reversed(range(chips)):
        total = core_sum(r)
        arrivals = received.pop(r, [])
        if r == 0:
            for arrival in arrivals[:-1]:
                total = total + arrival.astype(jnp.float32)
            return lead, after(total) + arrivals[-1].astype(jnp.float32)
        for arrival in arrivals:
            total = total + arrival.astype(jnp.float32)
        b = r.bit_length() - 1
        pairs = swapped(
            count, lambda i: (1 << b if i & 1 == 0 else 1 << (bits - 1 - b)) << 1
        )
        sent = total.astype(jnp.bfloat16)
        partner[r - 1] = after(partner[r - 1], sent)
        arrival = lax.ppermute(sent, "shard", pairs)
        received.setdefault(r - (1 << b), []).append(arrival)


def summed_over(value, axis, distances):
    size = lax.axis_size(axis)
    total = value
    for distance in distances:
        total = total + lax.ppermute(value, axis, swapped(size, lambda i: distance))
    return total


def step(grad_parts, params, moment_first, moment_second, block_layer, block_valid, decay):
    row_count = params.shape[1]
    n_shard = lax.axis_size("shard")
    n_section = lax.axis_size("section")
    lead, gradient = scattered_sum(grad_parts[0, 0], n_shard, row_count)
    block_layer, block_valid, _ = lax.optimization_barrier((block_layer, block_valid, lead))
    block_rows = row_count // block_layer.shape[1]
    layer_rows = jnp.repeat(block_layer[0], block_rows)
    valid_rows = jnp.repeat(block_valid[0], block_rows) > 0
    layer_ids = jnp.arange(decay.shape[0], dtype=jnp.int32)
    onehot = jnp.where(
        valid_rows[:, None] & (layer_rows[:, None] == layer_ids[None, :]), 1.0, 0.0
    ).astype(jnp.float32)
    weights = params[0].astype(jnp.float32)
    weight_sums = after(jnp.sum(weights * weights, axis=-1))
    row_decay = after(jnp.dot(onehot, decay, precision=lax.Precision.HIGHEST))
    first = 0.9 * moment_first[0] + 0.1 * gradient
    second = 0.99 * moment_second[0] + 0.01 * gradient * gradient
    update = (
        first / bias_first / (jnp.sqrt(second / bias_second) + 1e-06) + row_decay[:, None] * weights
    )
    row_sums = jnp.stack([weight_sums, jnp.sum(update * update, axis=-1)], axis=1)
    partial_value = jnp.dot(onehot.T, row_sums, precision=lax.Precision.HIGHEST)
    totals = summed_over(partial_value, "shard", (1,))
    late_gradient = after(gradient, totals)
    live = valid_rows[:, None]
    first = 0.9 * moment_first[0] + 0.1 * late_gradient
    second = 0.99 * moment_second[0] + 0.01 * late_gradient * late_gradient
    new_first = jnp.where(live, first, moment_first[0])
    new_second = jnp.where(live, second, moment_second[0])
    for b in range(1, bits_of(n_shard), 2):
        pair = (1 << b, 2 << b, 3 << b) if 2 << b < n_shard else (1 << b,)
        totals = summed_over(totals, "shard", pair)
    totals, new_first, new_second = lax.optimization_barrier((totals, new_first, new_second))
    for b in range(bits_of(n_section)):
        totals = summed_over(totals, "section", (1 << b,))
    ratios = jnp.sqrt(totals[:, 0] / (totals[:, 1] + 1.0))
    row_ratio = jnp.dot(onehot, ratios, precision=lax.Precision.HIGHEST)
    stepped = weights - 0.1 * row_ratio[:, None] * update
    new_params = jnp.where(live, stepped, weights).astype(jnp.bfloat16)
    return (new_params[None], new_first[None], new_second[None], ratios)


def solution(mesh):
    placed = (
        P("section", "shard", None, None),
        P("section", "shard", None),
        P("section", "shard", None),
        P("section", "shard", None),
        P("section", "shard"),
        P("section", "shard"),
        P(),
    )
    return jax.shard_map(
        step,
        mesh=mesh,
        in_specs=placed,
        out_specs=(
            P("section", "shard", None),
            P("section", "shard", None),
            P("section", "shard", None),
            P(),
        ),
        check_vma=False,
    )
```
